32 devices in a mesh: groups: 2 (over x), seq: 16 (over z, y, core).
Axes of the slice: x: 2, y: 2, z: 4, core: 2. Of those that a mesh axis runs over, the one named last changes fastest.
Arguments:
- queries: bfloat16 [1024, 2048], P(('groups', 'seq')), parts along dimension 0, may hold values from -132 to 132
- fresh_keys: bfloat16 [1024, 2048], P(('groups', 'seq')), parts along dimension 0, may hold values from -6 to 6
- fresh_values: bfloat16 [1024, 2048], P(('groups', 'seq')), parts along dimension 0, may hold values from -48 to 48
- stale_keys: bfloat16 [1024, 2048], P(('groups', 'seq')), parts along dimension 0, may hold values from -6 to 6
- stale_values: bfloat16 [1024, 2048], P(('groups', 'seq')), parts along dimension 0, may hold values from -48 to 48
- patch_sizes: int32 [8], P('groups'), parts along dimension 0, may hold values from 1 to 256, 512 in all
Outputs:
- attended: bfloat16 [1024, 2048], P(('groups', 'seq')), parts along dimension 0
The draws below stay inside these ranges and needn't reach their ends.
There are 2 independent parts, one for each index of `groups`. The reference program is written for one: setup_inputs(seed, part) draws one part's arguments, and reference() takes and returns one part's arrays. A program takes and returns all parts, laid end to end along the dimension named above; each array names one. Nothing has to cross between parts.
Inputs may be any that keep to these rules, and one draw needn't show every extreme that they name: `patch_sizes`: the patch lengths sum to 512.
All inputs are finite; a program needn't handle non-finite values.
Results may differ from the reference program's by a relative error of at most 0.006.
Values may be sent and summed in bfloat16 or wider, within the bound.
No kernel may reach another device: no remote copies, remote signals or barrier semaphores. Data moves between devices by JAX's collectives and lax.ppermute only.
A program may use at most 64 MiB of HBM per device.

```python
import math
import jax
import jax.numpy as jnp
import numpy as np
from jax import lax

H = 16
HD = 128
PATCHES = 4
TOKENS = 512


def base_keys(key):
    return jnp.clip(jax.random.normal(jax.random.fold_in(key, 5), (TOKENS, H * HD), jnp.float32), -6.0, 6.0)


def draw_fresh_keys(key, part):
    return base_keys(key).astype(jnp.bfloat16)


def draw_queries(key, part):
    drawn = jnp.clip(2.0 * jax.random.normal(jax.random.fold_in(key, 6), (TOKENS, H * HD), jnp.float32), -12.0, 12.0)
    return drawn.astype(jnp.bfloat16)


def block_levels(stream_key, shape, cuts, least, high):
    level = 1.0
    for axis_at, shards_of in cuts:
        steps = jax.random.uniform(jax.random.fold_in(jax.random.fold_in(stream_key, 6), axis_at), (shards_of,), jnp.float32, least / len(cuts), high / len(cuts))
        level = level * jnp.repeat(jnp.exp(steps), shape[axis_at] // shards_of).reshape((-1,) + (1,) * (len(shape) - 1 - axis_at))
    return level


def profile(number_of, total, limit, lean):
    loads = [(1 << 20) // math.isqrt(rank ** lean) + 1 for rank in range(2, number_of + 1)]
    spare, holding = total - limit - (number_of - 1), [1] * (number_of - 1)
    while spare > 0:
        free = [i for i in range(number_of - 1) if holding[i] < limit]
        mass, remaining = sum([loads[i] for i in free]), spare
        for i in free:
            more = min(limit - holding[i], max(1, remaining * loads[i] // mass), spare)
            holding[i] = holding[i] + more
            spare = spare - more
    return np.array([limit] + holding)


def ragged_sizes(rng, number_of, total, most, slope):
    if number_of == 2:
        one = jax.random.randint(rng, (), max(1, total - most), min(most, total - 1) + 1)
        return jnp.stack([one, total - one])
    sizes = jnp.asarray(profile(number_of, total, most, slope), jnp.int32)
    couples = (number_of - 1) // 2
    source_of, receiver = sizes[1:1 + 2 * couples:2], sizes[2:2 + 2 * couples:2]
    room = jnp.minimum(source_of - 1, most - receiver)
    moved = jax.random.randint(jax.random.fold_in(rng, 1), (couples,), 0, 1 << 20) % (room + 1)
    sizes = sizes.at[1:1 + 2 * couples:2].set(source_of - moved).at[2:2 + 2 * couples:2].set(receiver + moved)
    return sizes[jax.random.permutation(jax.random.fold_in(rng, 2), number_of)]


def scatter_about(own_key, extent, spread, bound, split=(), held_as=jnp.bfloat16):
    entries = jax.random.normal(own_key, extent, jnp.float32) * spread
    if len(split) > 0:
        entries = block_levels(own_key, extent, split, -0.22, 0.18) * entries
    return jnp.clip(entries, min=-bound, max=bound).astype(held_as)


def setup_inputs(seed: int = 0, part: int = 0) -> dict:
    arg_keys = jax.random.split(jax.random.key(seed), 7)
    part_keys = jax.random.split(jax.random.fold_in(arg_keys[6], part), 7)
    queries = draw_queries(jax.random.fold_in(jax.random.fold_in(arg_keys[6], part), 71), part)
    fresh_keys = draw_fresh_keys(jax.random.fold_in(jax.random.fold_in(arg_keys[6], part), 71), part)
    fresh_values = scatter_about(part_keys[2], (TOKENS, H * HD), 8.0, 48.0, ((0, 16),))
    stale_keys = scatter_about(part_keys[3], (TOKENS, H * HD), 1.0, 6.0, ((0, 16),))
    stale_values = scatter_about(part_keys[4], (TOKENS, H * HD), 8.0, 48.0, ((0, 16),))
    patch_sizes = ragged_sizes(part_keys[5], PATCHES, TOKENS, TOKENS // 2, 1).astype(jnp.int32)
    return dict(queries=queries, fresh_keys=fresh_keys, fresh_values=fresh_values, stale_keys=stale_keys, stale_values=stale_values, patch_sizes=patch_sizes)


def reference(queries, fresh_keys, fresh_values, stale_keys, stale_values, patch_sizes):
    total_rows, columns = queries.shape
    head_size = columns // H
    block_rows = math.gcd(total_rows, 512)
    patch_ends = jnp.cumsum(patch_sizes)[:-1]
    positions = jnp.arange(total_rows, dtype=jnp.int32)
    token_patch = jnp.sum((positions[:, None] >= patch_ends[None, :]).astype(jnp.int32), axis=1)
    score_scale = head_size ** -0.5

    def one_head(head):
        start = (head * head_size).astype(jnp.int32)

        def take(array):
            return lax.dynamic_slice_in_dim(array, start, head_size, 1)

        query_head = take(queries).reshape(-1, block_rows, head_size)
        key_fresh = take(fresh_keys)
        value_fresh = take(fresh_values)
        key_stale = take(stale_keys)
        value_stale = take(stale_values)
        patch_blocks = token_patch.reshape(-1, block_rows)

        def one_block(pair):
            query_block, query_patch = pair
            is_fresh = token_patch[None, :] <= query_patch[:, None]
            fresh_scores = jnp.dot(query_block, key_fresh.T, preferred_element_type=jnp.float32)
            stale_scores = jnp.dot(query_block, key_stale.T, preferred_element_type=jnp.float32)
            scores = jnp.where(is_fresh, fresh_scores, stale_scores) * score_scale
            weights = jnp.exp(scores - jnp.max(scores, axis=1, keepdims=True))
            denominator = jnp.sum(weights, axis=1, keepdims=True)
            rounded = weights.astype(jnp.bfloat16)
            zeroes = jnp.zeros_like(rounded)
            numerator = jnp.dot(jnp.where(is_fresh, rounded, zeroes), value_fresh, preferred_element_type=jnp.float32)
            numerator = numerator + jnp.dot(jnp.where(is_fresh, zeroes, rounded), value_stale, preferred_element_type=jnp.float32)
            return (numerator / denominator).astype(jnp.bfloat16)

        return lax.map(one_block, (query_head, patch_blocks)).reshape(total_rows, head_size)

    heads_out = lax.map(one_head, jnp.arange(H, dtype=jnp.int32))
    return jnp.transpose(heads_out, (1, 0, 2)).reshape(total_rows, columns)
```

```python
import functools
import math

import jax
import jax.numpy as jnp
from jax import lax
from jax.experimental import pallas as pl
from jax.experimental.pallas import tpu as pltpu
from jax.sharding import PartitionSpec as P

H = 16
ARRAYS = 5
CONTRACT = (((1,), (1,)), ((), ()))


def attend(groups, meta_ref, *refs):
    blocks, out_ref = refs[:groups], refs[groups]
    runs, _, run_rows, head_size = blocks[0].shape
    rows = runs * run_rows
    patches = meta_ref.shape[0]
    base = head_size ** (-0.5) * math.log2(math.e)

    def flat(ref, which):
        return ref[:, which].reshape(rows, head_size)

    own_group = meta_ref[patches - 1]
    query_at = lax.broadcasted_iota(jnp.int32, (rows, 1), 0) * groups + own_group
    bound = jnp.full((rows, 1), rows * groups, jnp.int32)
    for p in reversed(range(patches - 1)):
        bound = jnp.where(query_at < meta_ref[p], meta_ref[p], bound)

    queries = flat(blocks[0], 0)
    top = total = acc = None
    for offset in range(groups):
        ref = blocks[offset]
        first = 1 if offset == 0 else 0
        source = lax.rem(own_group - offset + groups, groups)
        key_at = lax.broadcasted_iota(jnp.int32, (1, rows), 1) * groups + source
        is_fresh = key_at < bound
        fresh = lax.dot_general(
            queries, flat(ref, first), CONTRACT, preferred_element_type=jnp.float32
        )
        stale = lax.dot_general(
            queries, flat(ref, first + 2), CONTRACT, preferred_element_type=jnp.float32
        )
        scores = jnp.where(is_fresh, fresh, stale)
        block_top = jnp.max(scores, axis=1, keepdims=True)
        new_top = block_top if top is None else jnp.maximum(top, block_top)
        weights = jnp.exp2((scores - new_top) * base)
        block_total = jnp.sum(weights, axis=1, keepdims=True)
        zeroes = jnp.zeros_like(weights)
        part = jnp.dot(
            jnp.where(is_fresh, weights, zeroes).astype(jnp.bfloat16),
            flat(ref, first + 1),
            preferred_element_type=jnp.float32,
        ) + jnp.dot(
            jnp.where(is_fresh, zeroes, weights).astype(jnp.bfloat16),
            flat(ref, first + 3),
            preferred_element_type=jnp.float32,
        )
        if top is None:
            total, acc = block_total, part
        else:
            rescale = jnp.exp2((top - new_top) * base)
            total = total * rescale + block_total
            acc = acc * rescale + part
        top = new_top
    out_ref[...] = (acc / total).astype(out_ref.dtype).reshape(out_ref.shape)


def shards(queries, fresh_keys, fresh_values, stale_keys, stale_values, patch_sizes):
    local_rows, columns = queries.shape
    head_size = columns // H
    devices = lax.axis_size("seq")
    groups = devices // H
    sub_rows = local_rows // groups
    packed = jnp.stack(
        [
            x.reshape(sub_rows, devices, head_size).transpose(1, 0, 2)
            for x in (queries, fresh_keys, fresh_values, stale_keys, stale_values)
        ],
        axis=1,
    )
    moved = lax.all_to_all(packed, "seq", split_axis=0, concat_axis=0, tiled=True)
    if sub_rows % 16:
        moved = moved.transpose(1, 0, 2, 3).reshape(1, ARRAYS, devices * sub_rows, head_size)
    own_group = lax.axis_index("seq") // H
    meta = jnp.concatenate([jnp.cumsum(patch_sizes)[:-1], own_group[None]]).astype(jnp.int32)
    blocks = [moved]
    travelling = moved[:, 1:]
    for _ in range(1, groups):
        route = [((i - H) % devices, i) for i in range(devices)]
        travelling = lax.ppermute(travelling, "seq", route)
        blocks.append(travelling)
    attended = pl.pallas_call(
        functools.partial(attend, groups),
        out_shape=jax.ShapeDtypeStruct(moved.shape[:1] + moved.shape[2:], jnp.bfloat16),
        in_specs=[pl.BlockSpec(memory_space=pltpu.SMEM)]
        + [pl.BlockSpec(memory_space=pltpu.VMEM)] * groups,
        out_specs=pl.BlockSpec(memory_space=pltpu.VMEM),
        compiler_params=pltpu.CompilerParams(vmem_limit_bytes=48 * 1024 * 1024),
        name="attend",
    )(meta, *blocks)
    returned = lax.all_to_all(
        attended.reshape(devices, sub_rows, head_size),
        "seq",
        split_axis=0,
        concat_axis=0,
        tiled=True,
    )
    return returned.transpose(1, 0, 2).reshape(local_rows, columns)


def solution(mesh):
    spec = P(("groups", "seq"), None)
    in_specs = (spec, spec, spec, spec, spec, P("groups"))
    return jax.shard_map(shards, mesh=mesh, in_specs=in_specs, out_specs=spec, check_vma=False)
```

```python
import functools
import math

import jax
import jax.numpy as jnp
from jax import lax
from jax.experimental import pallas as pl
from jax.experimental.pallas import tpu as pltpu
from jax.sharding import PartitionSpec as P

H = 16
ARRAYS = 5
CONTRACT = (((1,), (1,)), ((), ()))


def attend(groups, sizes_ref, *refs):
    blocks, out_ref = refs[:groups], refs[groups]
    runs, _, run_rows, head_size = blocks[0].shape
    rows = runs * run_rows
    ends = [sizes_ref[0]]
    for p in range(1, sizes_ref.shape[0] - 1):
        ends.append(ends[-1] + sizes_ref[p])
    base = head_size ** (-0.5) * math.log2(math.e)

    def flat(ref, which):
        return ref[:, which].reshape(rows, head_size)

    own_group = lax.axis_index("seq") // H
    query_at = lax.broadcasted_iota(jnp.int32, (rows, 1), 0) * groups + own_group
    bound = jnp.full((rows, 1), rows * groups, jnp.int32)
    for end in reversed(ends):
        bound = jnp.where(query_at < end, end, bound)

    queries = flat(blocks[0], 0)
    top = total = acc = None
    for offset in range(groups):
        ref = blocks[offset]
        first = 1 if offset == 0 else 0
        source = lax.rem(own_group - offset + groups, groups)
        key_at = lax.broadcasted_iota(jnp.int32, (1, rows), 1) * groups + source
        is_fresh = key_at < bound
        fresh = lax.dot_general(
            queries, flat(ref, first), CONTRACT, preferred_element_type=jnp.float32
        )
        stale = lax.dot_general(
            queries, flat(ref, first + 2), CONTRACT, preferred_element_type=jnp.float32
        )
        scores = jnp.where(is_fresh, fresh, stale)
        block_top = jnp.max(scores, axis=1, keepdims=True)
        new_top = block_top if top is None else jnp.maximum(top, block_top)
        weights = jnp.exp2((scores - new_top) * base)
        block_total = jnp.sum(weights, axis=1, keepdims=True)
        zeroes = jnp.zeros_like(weights)
        part = jnp.dot(
            jnp.where(is_fresh, weights, zeroes).astype(jnp.bfloat16),
            flat(ref, first + 1),
            preferred_element_type=jnp.float32,
        ) + jnp.dot(
            jnp.where(is_fresh, zeroes, weights).astype(jnp.bfloat16),
            flat(ref, first + 3),
            preferred_element_type=jnp.float32,
        )
        if top is None:
            total, acc = block_total, part
        else:
            rescale = jnp.exp2((top - new_top) * base)
            total = total * rescale + block_total
            acc = acc * rescale + part
        top = new_top
    out_ref[...] = (acc / total).astype(out_ref.dtype).reshape(out_ref.shape)


def pack(*refs):
    sources, out_ref, staged, arrived = refs[:ARRAYS], *refs[ARRAYS:]
    head_size = out_ref.shape[-1]
    copies = [
        pltpu.make_async_copy(source, staged.at[a], arrived.at[a])
        for a, source in enumerate(sources)
    ]
    for copy in copies:
        copy.start()
    for a, copy in enumerate(copies):
        copy.wait()
        for d in range(out_ref.shape[0]):
            out_ref[d, a] = staged[a, :, d * head_size : (d + 1) * head_size]


def shards(queries, fresh_keys, fresh_values, stale_keys, stale_values, patch_sizes):
    local_rows, columns = queries.shape
    head_size = columns // H
    devices = lax.axis_size("seq")
    groups = devices // H
    sub_rows = local_rows // groups
    arrays = (queries, fresh_keys, fresh_values, stale_keys, stale_values)
    if groups == 1 and sub_rows % 16 == 0:
        packed = pl.pallas_call(
            pack,
            out_shape=jax.ShapeDtypeStruct(
                (devices, ARRAYS, sub_rows, head_size), queries.dtype
            ),
            in_specs=[pl.BlockSpec(memory_space=pl.ANY)] * ARRAYS,
            out_specs=pl.BlockSpec(memory_space=pltpu.VMEM),
            scratch_shapes=[
                pltpu.VMEM((ARRAYS, local_rows, columns), queries.dtype),
                pltpu.SemaphoreType.DMA((ARRAYS,)),
            ],
            name="pack",
        )(*arrays)
    else:
        packed = jnp.stack(
            [x.reshape(sub_rows, devices, head_size).transpose(1, 0, 2) for x in arrays],
            axis=1,
        )
    moved = lax.all_to_all(packed, "seq", split_axis=0, concat_axis=0, tiled=True)
    if sub_rows % 16:
        moved = moved.transpose(1, 0, 2, 3).reshape(1, ARRAYS, devices * sub_rows, head_size)
    blocks = [moved]
    travelling = moved[:, 1:]
    for _ in range(1, groups):
        route = [((i - H) % devices, i) for i in range(devices)]
        travelling = lax.ppermute(travelling, "seq", route)
        blocks.append(travelling)
    attended = pl.pallas_call(
        functools.partial(attend, groups),
        out_shape=jax.ShapeDtypeStruct(moved.shape[:1] + moved.shape[2:], jnp.bfloat16),
        in_specs=[pl.BlockSpec(memory_space=pltpu.SMEM)]
        + [pl.BlockSpec(memory_space=pltpu.VMEM)] * groups,
        out_specs=pl.BlockSpec(memory_space=pltpu.VMEM),
        compiler_params=pltpu.CompilerParams(vmem_limit_bytes=48 * 1024 * 1024),
        name="attend",
    )(patch_sizes, *blocks)
    returned = lax.all_to_all(
        attended.reshape(devices, sub_rows, head_size),
        "seq",
        split_axis=0,
        concat_axis=0,
        tiled=True,
    )
    return returned.transpose(1, 0, 2).reshape(local_rows, columns)


def solution(mesh):
    spec = P(("groups", "seq"), None)
    in_specs = (spec, spec, spec, spec, spec, P("groups"))
    return jax.shard_map(shards, mesh=mesh, in_specs=in_specs, out_specs=spec, check_vma=False)
```

```python
import functools
import math

import jax
import jax.numpy as jnp
from jax import lax
from jax.experimental import pallas as pl
from jax.experimental.pallas import tpu as pltpu
from jax.sharding import PartitionSpec as P

H = 16
ARRAYS = 5
CHUNKS = 2
CONTRACT = (((1,), (1,)), ((), ()))


def attend(groups, sizes_ref, *refs):
    blocks, out_ref = refs[:groups], refs[groups]
    runs, _, run_rows, head_size = blocks[0].shape
    rows = runs * run_rows
    ends = [sizes_ref[0]]
    for p in range(1, sizes_ref.shape[0] - 1):
        ends.append(ends[-1] + sizes_ref[p])
    base = head_size ** (-0.5) * math.log2(math.e)

    def flat(ref, which):
        return ref[:, which].reshape(rows, head_size)

    own_group = lax.axis_index("seq") // H
    query_at = lax.broadcasted_iota(jnp.int32, (rows, 1), 0) * groups + own_group
    bound = jnp.full((rows, 1), rows * groups, jnp.int32)
    for end in reversed(ends):
        bound = jnp.where(query_at < end, end, bound)

    chunk = rows // CHUNKS
    for at in range(0, rows, chunk):
        queries = flat(blocks[0], 0)[at : at + chunk]
        edge = bound[at : at + chunk]
        top = total = acc = None
        for offset in range(groups):
            ref = blocks[offset]
            first = 1 if offset == 0 else 0
            source = lax.rem(own_group - offset + groups, groups)
            key_at = lax.broadcasted_iota(jnp.int32, (1, rows), 1) * groups + source
            is_fresh = key_at < edge
            fresh = lax.dot_general(
                queries, flat(ref, first), CONTRACT, preferred_element_type=jnp.float32
            )
            stale = lax.dot_general(
                queries, flat(ref, first + 2), CONTRACT, preferred_element_type=jnp.float32
            )
            scores = jnp.where(is_fresh, fresh, stale)
            block_top = jnp.max(scores, axis=1, keepdims=True)
            new_top = block_top if top is None else jnp.maximum(top, block_top)
            weights = jnp.exp2((scores - new_top) * base)
            block_total = jnp.sum(weights, axis=1, keepdims=True)
            zeroes = jnp.zeros_like(weights)
            part = jnp.dot(
                jnp.where(is_fresh, weights, zeroes).astype(jnp.bfloat16),
                flat(ref, first + 1),
                preferred_element_type=jnp.float32,
            ) + jnp.dot(
                jnp.where(is_fresh, zeroes, weights).astype(jnp.bfloat16),
                flat(ref, first + 3),
                preferred_element_type=jnp.float32,
            )
            if top is None:
                total, acc = block_total, part
            else:
                rescale = jnp.exp2((top - new_top) * base)
                total = total * rescale + block_total
                acc = acc * rescale + part
            top = new_top
        done = (acc / total).astype(out_ref.dtype)
        if run_rows == rows:
            out_ref[0, at : at + chunk] = done
        else:
            out_ref[at // run_rows : (at + chunk) // run_rows] = done.reshape(
                chunk // run_rows, run_rows, head_size
            )


def pack(*refs):
    sources, out_ref, staged, arrived = refs[:ARRAYS], *refs[ARRAYS:]
    head_size = out_ref.shape[-1]
    copies = [
        pltpu.make_async_copy(source, staged.at[a], arrived.at[a])
        for a, source in enumerate(sources)
    ]
    for copy in copies:
        copy.start()
    for a, copy in enumerate(copies):
        copy.wait()
        for d in range(out_ref.shape[0]):
            out_ref[d, a] = staged[a, :, d * head_size : (d + 1) * head_size]


def shards(queries, fresh_keys, fresh_values, stale_keys, stale_values, patch_sizes):
    local_rows, columns = queries.shape
    head_size = columns // H
    devices = lax.axis_size("seq")
    groups = devices // H
    sub_rows = local_rows // groups
    arrays = (queries, fresh_keys, fresh_values, stale_keys, stale_values)
    if groups == 1 and sub_rows % 16 == 0:
        packed = pl.pallas_call(
            pack,
            out_shape=pltpu.VMEM((devices, ARRAYS, sub_rows, head_size), queries.dtype),
            in_specs=[pl.BlockSpec(memory_space=pl.ANY)] * ARRAYS,
            out_specs=pl.BlockSpec(memory_space=pltpu.VMEM),
            scratch_shapes=[
                pltpu.VMEM((ARRAYS, local_rows, columns), queries.dtype),
                pltpu.SemaphoreType.DMA((ARRAYS,)),
            ],
            name="pack",
        )(*arrays)
    else:
        packed = jnp.stack(
            [x.reshape(sub_rows, devices, head_size).transpose(1, 0, 2) for x in arrays],
            axis=1,
        )
    moved = lax.all_to_all(packed, "seq", split_axis=0, concat_axis=0, tiled=True)
    if sub_rows % 16:
        moved = moved.transpose(1, 0, 2, 3).reshape(1, ARRAYS, devices * sub_rows, head_size)
    blocks = [moved]
    travelling = moved[:, 1:]
    for _ in range(1, groups):
        route = [((i - H) % devices, i) for i in range(devices)]
        travelling = lax.ppermute(travelling, "seq", route)
        blocks.append(travelling)
    attended = pl.pallas_call(
        functools.partial(attend, groups),
        out_shape=jax.ShapeDtypeStruct(moved.shape[:1] + moved.shape[2:], jnp.bfloat16),
        in_specs=[pl.BlockSpec(memory_space=pltpu.SMEM)]
        + [pl.BlockSpec(memory_space=pltpu.VMEM)] * groups,
        out_specs=pl.BlockSpec(memory_space=pltpu.VMEM),
        compiler_params=pltpu.CompilerParams(vmem_limit_bytes=48 * 1024 * 1024),
        name="attend",
    )(patch_sizes, *blocks)
    returned = lax.all_to_all(
        attended.reshape(devices, sub_rows, head_size),
        "seq",
        split_axis=0,
        concat_axis=0,
        tiled=True,
    )
    return returned.transpose(1, 0, 2).reshape(local_rows, columns)


def solution(mesh):
    spec = P(("groups", "seq"), None)
    in_specs = (spec, spec, spec, spec, spec, P("groups"))
    return jax.shard_map(shards, mesh=mesh, in_specs=in_specs, out_specs=spec, check_vma=False)
```

```python
import functools
import math

import jax
import jax.numpy as jnp
from jax import lax
from jax.experimental import pallas as pl
from jax.experimental.pallas import tpu as pltpu
from jax.sharding import PartitionSpec as P

H = 16
ARRAYS = 5
CHUNKS = 1
CONTRACT = (((1,), (1,)), ((), ()))


def attend(groups, sizes_ref, *refs):
    blocks, out_ref = refs[:groups], refs[groups]
    runs, _, run_rows, head_size = blocks[0].shape
    rows = runs * run_rows
    ends = [sizes_ref[0]]
    for p in range(1, sizes_ref.shape[0] - 1):
        ends.append(ends[-1] + sizes_ref[p])
    base = head_size ** (-0.5) * math.log2(math.e)

    def flat(ref, which):
        return ref[:, which].reshape(rows, head_size)

    own_group = lax.axis_index("seq") // H
    query_at = lax.broadcasted_iota(jnp.int32, (1, rows), 1) * groups + own_group
    bound = jnp.full((1, rows), rows * groups, jnp.int32)
    for end in reversed(ends):
        bound = jnp.where(query_at < end, end, bound)

    chunk = rows // CHUNKS
    for at in range(0, rows, chunk):
        queries = flat(blocks[0], 0)[at : at + chunk]
        edge = bound[:, at : at + chunk]
        top = total = acc = None
        for offset in range(groups):
            ref = blocks[offset]
            first = 1 if offset == 0 else 0
            source = lax.rem(own_group - offset + groups, groups)
            key_at = lax.broadcasted_iota(jnp.int32, (rows, 1), 0) * groups + source
            is_fresh = key_at < edge
            fresh = lax.dot_general(
                flat(ref, first), queries, CONTRACT, preferred_element_type=jnp.float32
            )
            stale = lax.dot_general(
                flat(ref, first + 2), queries, CONTRACT, preferred_element_type=jnp.float32
            )
            scores = jnp.where(is_fresh, fresh, stale)
            block_top = jnp.max(scores, axis=0, keepdims=True)
            new_top = block_top if top is None else jnp.maximum(top, block_top)
            weights = jnp.exp2((scores - new_top) * base)
            block_total = jnp.sum(weights, axis=0, keepdims=True)
            zeroes = jnp.zeros_like(weights)
            part = jnp.dot(
                flat(ref, first + 1).T,
                jnp.where(is_fresh, weights, zeroes).astype(jnp.bfloat16),
                preferred_element_type=jnp.float32,
            ) + jnp.dot(
                flat(ref, first + 3).T,
                jnp.where(is_fresh, zeroes, weights).astype(jnp.bfloat16),
                preferred_element_type=jnp.float32,
            )
            if top is None:
                total, acc = block_total, part
            else:
                rescale = jnp.exp2((top - new_top) * base)
                total = total * rescale + block_total
                acc = acc * rescale + part
            top = new_top
        done = (acc / total).T.astype(out_ref.dtype)
        if run_rows == rows:
            out_ref[0, at : at + chunk] = done
        else:
            out_ref[at // run_rows : (at + chunk) // run_rows] = done.reshape(
                chunk // run_rows, run_rows, head_size
            )


def pack(*refs):
    sources, out_ref, staged, arrived = refs[:ARRAYS], *refs[ARRAYS:]
    head_size = out_ref.shape[-1]
    copies = [
        pltpu.make_async_copy(source, staged.at[a], arrived.at[a])
        for a, source in enumerate(sources)
    ]
    for copy in copies:
        copy.start()
    for a, copy in enumerate(copies):
        copy.wait()
        for d in range(out_ref.shape[0]):
            out_ref[d, a] = staged[a, :, d * head_size : (d + 1) * head_size]


def shards(queries, fresh_keys, fresh_values, stale_keys, stale_values, patch_sizes):
    local_rows, columns = queries.shape
    head_size = columns // H
    devices = lax.axis_size("seq")
    groups = devices // H
    sub_rows = local_rows // groups
    arrays = (queries, fresh_keys, fresh_values, stale_keys, stale_values)
    if groups == 1 and sub_rows % 16 == 0:
        packed = pl.pallas_call(
            pack,
            out_shape=pltpu.VMEM((devices, ARRAYS, sub_rows, head_size), queries.dtype),
            in_specs=[pl.BlockSpec(memory_space=pl.ANY)] * ARRAYS,
            out_specs=pl.BlockSpec(memory_space=pltpu.VMEM),
            scratch_shapes=[
                pltpu.VMEM((ARRAYS, local_rows, columns), queries.dtype),
                pltpu.SemaphoreType.DMA((ARRAYS,)),
            ],
            name="pack",
        )(*arrays)
    else:
        packed = jnp.stack(
            [x.reshape(sub_rows, devices, head_size).transpose(1, 0, 2) for x in arrays],
            axis=1,
        )
    moved = lax.all_to_all(packed, "seq", split_axis=0, concat_axis=0, tiled=True)
    if sub_rows % 16:
        moved = moved.transpose(1, 0, 2, 3).reshape(1, ARRAYS, devices * sub_rows, head_size)
    blocks = [moved]
    travelling = moved[:, 1:]
    for _ in range(1, groups):
        route = [((i - H) % devices, i) for i in range(devices)]
        travelling = lax.ppermute(travelling, "seq", route)
        blocks.append(travelling)
    attended = pl.pallas_call(
        functools.partial(attend, groups),
        out_shape=jax.ShapeDtypeStruct(moved.shape[:1] + moved.shape[2:], jnp.bfloat16),
        in_specs=[pl.BlockSpec(memory_space=pltpu.SMEM)]
        + [pl.BlockSpec(memory_space=pltpu.VMEM)] * groups,
        out_specs=pl.BlockSpec(memory_space=pltpu.VMEM),
        compiler_params=pltpu.CompilerParams(vmem_limit_bytes=48 * 1024 * 1024),
        name="attend",
    )(patch_sizes, *blocks)
    returned = lax.all_to_all(
        attended.reshape(devices, sub_rows, head_size),
        "seq",
        split_axis=0,
        concat_axis=0,
        tiled=True,
    )
    return returned.transpose(1, 0, 2).reshape(local_rows, columns)


def solution(mesh):
    spec = P(("groups", "seq"), None)
    in_specs = (spec, spec, spec, spec, spec, P("groups"))
    return jax.shard_map(shards, mesh=mesh, in_specs=in_specs, out_specs=spec, check_vma=False)
```
